1024 devices in a mesh: grp: 4 (over x), row: 16 (over y, core), col: 16 (over z).
Axes of the slice: x: 4, y: 8, z: 16, core: 2. Of those that a mesh axis runs over, the one named last changes fastest.
Arguments:
- gradients: bfloat16 [4, 3072, 24576], P('grp', 'row', 'col'), may hold values from -6 to 6
- momentum: float32 [4, 3072, 24576], P('grp', 'row', 'col'), may hold values from -94 to 94, as said below
- right_basis: bfloat16 [24576, 512], P('col'), may hold values from -6 to 6
Outputs:
- new_momentum: float32 [4, 3072, 24576], P('grp', 'row', 'col')
- new_basis: bfloat16 [24576, 512], P('col')
- update: bfloat16 [3072, 24576], P('row', 'col')
The draws below stay inside these ranges and needn't reach their ends.
Inputs may be any that keep to these rules, and one draw needn't show every extreme that they name: Each group's momentum buffer holds real values bounded in magnitude by 94.
All inputs are finite; a program needn't handle non-finite values.
Results may differ from the reference program's by a relative error of at most 0.013.
Values may be sent and summed in bfloat16 or wider, within the bound.
A program may use at most 32 MiB of HBM per device.

```python
import math
import jax
import jax.numpy as jnp
from jax import lax

D = 3072
FF = 24576
R = 512
GROUPS = 4


def draw_momentum(key, part):
    keys = jax.random.split(jax.random.fold_in(key, 17), 4)
    row_scale = jnp.exp(jax.random.uniform(keys[0], (D,), jnp.float32, math.log(0.3), math.log(3.0)))
    position = jnp.arange(FF, dtype=jnp.float32) / FF
    col_scale = jnp.exp(jax.random.uniform(keys[1], (FF,), jnp.float32, math.log(0.3), math.log(3.0))) * jnp.exp(math.log(3.0) * (position - 0.5))
    common = jax.random.normal(keys[2], (1, D, FF), jnp.float32)
    own = jax.random.normal(keys[3], (GROUPS, D, FF), jnp.float32)
    mixed = 0.8 * common + 0.6 * own
    mixed = jnp.clip(mixed, -6.0, 6.0)
    return (mixed * row_scale[None, :, None] * col_scale[None, None, :]).astype(jnp.float32)


def block_levels(key, extent, cuts, low, largest):
    factor_of = 1.0
    for dim, parts in cuts:
        draws = jax.random.uniform(jax.random.fold_in(jax.random.fold_in(key, 6), dim), (parts,), jnp.float32, low / len(cuts), largest / len(cuts))
        factor_of = factor_of * jnp.repeat(jnp.exp(draws), extent[dim] // parts).reshape((-1,) + (1,) * (len(extent) - 1 - dim))
    return factor_of


def gaussian(key, dims, spread, bound, cuts=(), kind=jnp.bfloat16):
    result = jax.random.normal(key, dims, jnp.float32) * spread
    if len(cuts) > 0:
        result = block_levels(key, dims, cuts, -0.22, 0.18) * result
    return jnp.clip(result, min=-bound, max=bound).astype(kind)


def setup_inputs(seed: int = 0) -> dict:
    seeds = jax.random.split(jax.random.key(seed), 4)
    return {
        "gradients": gaussian(seeds[0], (GROUPS, D, FF), 1.0, 6.0, ((0, 4), (1, 16), (2, 16))),
        "momentum": draw_momentum(jax.random.fold_in(seeds[3], 71), 0),
        "right_basis": gaussian(seeds[2], (FF, R), 1.0, 6.0, ((0, 16),)),
    }


momentum_decay = 0.9
ridge_scale = 0.0001
epsilon = 1e-06

def reference(gradients, momentum, right_basis):
    left_factor = jnp.zeros((D, R), jnp.float32)
    for group in range(GROUPS):
        merged_low = (momentum[group] + gradients[group].astype(jnp.float32)).astype(jnp.bfloat16)
        left_factor = left_factor + jnp.dot(merged_low.astype(jnp.float32), right_basis.astype(jnp.float32), preferred_element_type=jnp.float32)
    gram_matrix = jnp.dot(left_factor.T.astype(jnp.float32), left_factor.astype(jnp.float32), precision=lax.Precision.HIGHEST, preferred_element_type=jnp.float32)
    shifted = gram_matrix + ridge_scale * (jnp.trace(gram_matrix) / R) * jnp.eye(R, dtype=jnp.float32)
    cholesky_factor = jnp.linalg.cholesky(shifted)
    orthonormal = jax.scipy.linalg.solve_triangular(cholesky_factor, left_factor.T, lower=True).T
    orthonormal_low = orthonormal.astype(jnp.bfloat16)
    right_factor = jnp.zeros((FF, R), jnp.float32)
    for group in range(GROUPS):
        merged_low = (momentum[group] + gradients[group].astype(jnp.float32)).astype(jnp.bfloat16)
        right_factor = right_factor + jnp.dot(merged_low.T.astype(jnp.float32), orthonormal_low.astype(jnp.float32), preferred_element_type=jnp.float32)
    right_factor = right_factor / GROUPS
    column_rms = jnp.sqrt(lax.optimization_barrier(jnp.sum(right_factor * right_factor, axis=0)) / FF + epsilon)
    new_basis = (right_factor / column_rms).astype(jnp.bfloat16)
    scaled_low = (orthonormal * column_rms).astype(jnp.bfloat16)
    update = (math.sqrt(D / R) * jnp.dot(orthonormal_low.astype(jnp.float32), new_basis.T.astype(jnp.float32), preferred_element_type=jnp.float32)).astype(jnp.bfloat16)
    feedback = jnp.dot(scaled_low.astype(jnp.float32), new_basis.T.astype(jnp.float32), preferred_element_type=jnp.float32)
    outputs = []
    for group in range(GROUPS):
        merged = momentum[group] + gradients[group].astype(jnp.float32)
        outputs.append(merged - (1 - momentum_decay) * feedback)
    return (jnp.stack(outputs), new_basis, update)
```

```python
import functools
import math

import jax
import jax.numpy as jnp
from jax import lax
from jax.experimental import pallas as pl
from jax.experimental.pallas import tpu as pltpu
from jax.sharding import Mesh
from jax.sharding import PartitionSpec as P

MESH = pl.DeviceIdType.MESH
X, Y, K, Z = "grp", "row_0", "row_1", "col"
ROW = (Y, K)

momentum_decay = 0.9
ridge_scale = 0.0001
epsilon = 1e-06


def peer_of(axis, offset):
    return lax.rem(lax.axis_index(axis) + offset, lax.axis_size(axis))


def meet(axes):
    barrier = pltpu.get_barrier_semaphore()
    count = 0
    for axis in axes:
        for j in range(1, lax.axis_size(axis)):
            pl.semaphore_signal(barrier, inc=1, device_id={axis: peer_of(axis, j)}, device_id_type=MESH)
            count += 1
    return lambda: pl.semaphore_wait(barrier, count)


def send(src, dst, send_sem, recv_sem, axis, peer):
    copy = pltpu.make_async_remote_copy(
        src_ref=src, dst_ref=dst, send_sem=send_sem, recv_sem=recv_sem,
        device_id={axis: peer}, device_id_type=MESH,
    )
    copy.start()
    return copy


def scatter(tiles, arrived, sems, axis):
    copies = []
    for j in range(1, lax.axis_size(axis)):
        peer = peer_of(axis, j)
        copies.append(send(tiles.at[peer], arrived.at[j - 1], sems.at[0, j - 1], sems.at[1, j - 1], axis, peer))
    return copies


def share(slot, sems, axis):
    return [
        send(slot, slot, sems.at[0, j - 1], sems.at[1, j - 1], axis, peer_of(axis, j))
        for j in range(1, lax.axis_size(axis))
    ]


def arrive(copies):
    for copy in copies:
        copy.wait_recv()


def depart(copies):
    for copy in copies:
        copy.wait_send()


def left_kernel(
    mom, grad, basis, gram, left, low, part, xin, zpart, zin, lall, gall, gpair, kin, yall, gfull,
    sx, sz, sza, sxa, sk, sy, sgz, sgx, sgk,
):
    nx, ny, nz = lax.axis_size(X), lax.axis_size(Y), lax.axis_size(Z)
    g, y, k, c = (lax.axis_index(a) for a in (X, Y, K, Z))
    gathered = meet((X, Y, K, Z))
    rows = mom.shape[0]
    lanes = part.shape[2]
    fours = zpart.shape[1]
    merged_low = (mom[...] + grad[...].astype(jnp.float32)).astype(jnp.bfloat16)
    low[...] = merged_low
    product = jnp.dot(merged_low, basis[...], preferred_element_type=jnp.float32)
    for b in range(nx):
        part[b] = product[:, b * lanes : (b + 1) * lanes]
    gathered()
    sent = scatter(part, xin, sx, X)
    pending = list(sent)
    arrive(sent)
    total = part[g]
    for j in range(nx - 1):
        total = total + xin[j]
    for q in range(rows // 4):
        zpart[q // fours, q % fours] = total[4 * q : 4 * q + 4]
    sent = scatter(zpart, zin, sz, Z)
    pending += sent
    arrive(sent)
    own = zpart[c]
    for j in range(nz - 1):
        own = own + zin[j]
    lall[g, c] = own
    sent = share(lall.at[g, c], sza, Z)
    pending += sent
    arrive(sent)
    sent = share(lall.at[g], sxa, X)
    pending += sent
    arrive(sent)
    for b in range(nx):
        for q in range(rows // 4):
            left[4 * q : 4 * q + 4, b * lanes : (b + 1) * lanes] = lall[b, q // fours, q % fours]
    mine = left[:, pl.ds(pl.multiple_of(g * lanes, lanes), lanes)]
    gall[...] = lax.dot_general(
        mine, left[...], (((0,), (0,)), ((), ())),
        precision=lax.Precision.HIGHEST, preferred_element_type=jnp.float32,
    )
    strip = gall[pl.ds(pl.multiple_of(c * 8, 8), 8), :]
    half = strip.shape[1] // 2
    gpair[0] = strip[:, :half]
    gpair[1] = strip[:, half:]
    sent = scatter(gpair, kin, sk, K)
    pending += sent
    arrive(sent)
    yall[y] = gpair[k] + kin[0]
    sent = share(yall.at[y], sy, Y)
    pending += sent
    arrive(sent)
    total = yall[0]
    for j in range(1, ny):
        total = total + yall[j]
    gfull[k, g, c] = total
    sent = share(gfull.at[k, g, c], sgz, Z)
    pending += sent
    arrive(sent)
    sent = share(gfull.at[k, g], sgx, X)
    pending += sent
    arrive(sent)
    sent = share(gfull.at[k], sgk, K)
    pending += sent
    arrive(sent)
    for h in range(2):
        for b in range(nx):
            for q in range(nz):
                at = (b * nz + q) * 8
                gram[at : at + 8, h * half : (h + 1) * half] = gfull[h, b, q]
    depart(pending)


def left_call(mom, grad, basis):
    nx, ny, nz = lax.axis_size(X), lax.axis_size(Y), lax.axis_size(Z)
    rows, cols = mom.shape
    rank = basis.shape[1]
    lanes = rank // nx
    fours = rows // nz // 4
    half = rank // 2
    f32 = jnp.float32
    dma = lambda n: pltpu.SemaphoreType.DMA((2, n - 1))
    vmem = pl.BlockSpec(memory_space=pltpu.VMEM)
    return pl.pallas_call(
        left_kernel,
        out_shape=(
            jax.ShapeDtypeStruct((rank, rank), f32),
            jax.ShapeDtypeStruct((rows, rank), f32),
            jax.ShapeDtypeStruct((rows, cols), jnp.bfloat16),
        ),
        in_specs=[vmem] * 3,
        out_specs=(vmem,) * 3,
        scratch_shapes=[
            pltpu.VMEM((nx, rows, lanes), f32),
            pltpu.VMEM((nx - 1, rows, lanes), f32),
            pltpu.VMEM((nz, fours, 4, lanes), f32),
            pltpu.VMEM((nz - 1, fours, 4, lanes), f32),
            pltpu.VMEM((nx, nz, fours, 4, lanes), f32),
            pltpu.VMEM((lanes, rank), f32),
            pltpu.VMEM((2, 8, half), f32),
            pltpu.VMEM((1, 8, half), f32),
            pltpu.VMEM((ny, 8, half), f32),
            pltpu.VMEM((2, nx, nz, 8, half), f32),
            dma(nx), dma(nz), dma(nz), dma(nx), dma(2), dma(ny), dma(nz), dma(nx), dma(2),
        ],
        compiler_params=pltpu.CompilerParams(collective_id=0, has_side_effects=True),
        name="left",
    )(mom, grad, basis)


def right_kernel(
    groups, whole_rows, update_scale,
    mom, grad, low, orth, newmom, basis_out, update, ksend, kin, mine, xsend, xin, ysum, ysend, yin, nb, stack,
    qz, qk, qx, qy, sk, sx, sy, say, sax, sak, sqz, sqk, sqx, sqy,
):
    nx, ny, nz = lax.axis_size(X), lax.axis_size(Y), lax.axis_size(Z)
    g, y, k, c = (lax.axis_index(a) for a in (X, Y, K, Z))
    gathered = meet((X, Y, K, Z))
    rows, cols = mom.shape
    rank = orth.shape[1]
    half = cols // 2
    f32, bf16 = jnp.float32, jnp.bfloat16
    stack[:rows] = orth[...].astype(bf16)

    def product(at):
        return lax.dot_general(
            low[:, pl.ds(pl.multiple_of(at, 128), 128)], stack[:rows], (((0,), (0,)), ((), ())),
            preferred_element_type=f32,
        ) * (1.0 / groups)

    @pl.loop(0, half // 128)
    def _(i):
        ksend[pl.ds(pl.multiple_of(i * 128, 128), 128), :] = product((1 - k) * half + i * 128).astype(bf16)

    gathered()
    sent = [send(ksend, kin, sk.at[0, 0], sk.at[1, 0], K, 1 - k)]
    pending = list(sent)

    @pl.loop(0, half // 128)
    def _(i):
        mine[pl.ds(pl.multiple_of(i * 128, 128), 128), :] = product(k * half + i * 128)

    arrive(sent)
    block = half // nx
    for b in range(nx):
        at = slice(b * block, (b + 1) * block)
        both = mine[at] + kin[at].astype(f32)
        mine[at] = both
        xsend[b] = both.astype(bf16)
    sent = scatter(xsend, xin, sx, X)
    pending += sent
    arrive(sent)
    total = mine[pl.ds(pl.multiple_of(g * block, block), block), :]
    for j in range(nx - 1):
        total = total + xin[j].astype(f32)
    ysum[...] = total
    piece_rows = block // ny
    for b in range(ny):
        ysend[b] = total[b * piece_rows : (b + 1) * piece_rows].astype(bf16)
    sent = scatter(ysend, yin, sy, Y)
    pending += sent
    arrive(sent)
    piece = ysum[pl.ds(pl.multiple_of(y * piece_rows, 8), piece_rows), :]
    for j in range(ny - 1):
        piece = piece + yin[j].astype(f32)
    nb[k, g, y] = piece.astype(bf16)
    qz[c] = jnp.sum(piece * piece, axis=0, keepdims=True)
    sent_z = share(qz.at[c], sqz, Z)
    sent_y = share(nb.at[k, g, y], say, Y)
    pending += sent_z + sent_y

    def summed(ref, n):
        acc = ref[0]
        for j in range(1, n):
            acc = acc + ref[j]
        return acc

    arrive(sent_z)
    qk[k] = summed(qz, nz)
    sent = share(qk.at[k], sqk, K)
    pending += sent
    arrive(sent)
    qx[g] = summed(qk, 2)
    sent = share(qx.at[g], sqx, X)
    pending += sent
    arrive(sent_y)
    sent_x = share(nb.at[k, g], sax, X)
    pending += sent_x
    arrive(sent)
    qy[y] = summed(qx, nx)
    sent = share(qy.at[y], sqy, Y)
    pending += sent
    arrive(sent)
    squares = summed(qy, ny)
    column_rms = jnp.sqrt(squares / whole_rows + epsilon)
    inverse = 1.0 / column_rms
    stack[rows:] = (orth[...] * column_rms).astype(bf16)
    arrive(sent_x)
    sent = share(nb.at[k], sak, K)
    pending += sent
    arrive(sent)
    for h in range(2):
        for b in range(nx):
            for p in range(ny):
                at = h * half + b * block + p * piece_rows
                basis_out[at : at + piece_rows] = (nb[h, b, p].astype(f32) * inverse).astype(bf16)

    @pl.loop(0, cols // 256)
    def _(i):
        at = pl.ds(pl.multiple_of(i * 256, 256), 256)
        both = lax.dot_general(stack[...], basis_out[at, :], (((1,), (1,)), ((), ())), preferred_element_type=f32)
        update[:, at] = (update_scale * both[:rows]).astype(bf16)
        newmom[:, at] = mom[:, at] + grad[:, at].astype(f32) - (1 - momentum_decay) * both[rows:]

    depart(pending)


def right_call(mom, grad, low, orth, update_scale):
    nx, ny, nz = lax.axis_size(X), lax.axis_size(Y), lax.axis_size(Z)
    rows, cols = mom.shape
    rank = orth.shape[1]
    half = cols // 2
    block = half // nx
    piece = block // ny
    f32, bf16 = jnp.float32, jnp.bfloat16
    dma = lambda n: pltpu.SemaphoreType.DMA((2, n - 1))
    vmem = pl.BlockSpec(memory_space=pltpu.VMEM)
    return pl.pallas_call(
        functools.partial(right_kernel, nx, cols * nz, update_scale),
        out_shape=(
            jax.ShapeDtypeStruct((rows, cols), f32),
            jax.ShapeDtypeStruct((cols, rank), bf16),
            jax.ShapeDtypeStruct((rows, cols), bf16),
        ),
        in_specs=[vmem] * 4,
        out_specs=(vmem,) * 3,
        scratch_shapes=[
            pltpu.VMEM((half, rank), bf16),
            pltpu.VMEM((half, rank), bf16),
            pltpu.VMEM((half, rank), f32),
            pltpu.VMEM((nx, block, rank), bf16),
            pltpu.VMEM((nx - 1, block, rank), bf16),
            pltpu.VMEM((block, rank), f32),
            pltpu.VMEM((ny, piece, rank), bf16),
            pltpu.VMEM((ny - 1, piece, rank), bf16),
            pltpu.VMEM((2, nx, ny, piece, rank), bf16),
            pltpu.VMEM((2 * rows, rank), bf16),
            pltpu.VMEM((nz, 1, rank), f32),
            pltpu.VMEM((2, 1, rank), f32),
            pltpu.VMEM((nx, 1, rank), f32),
            pltpu.VMEM((ny, 1, rank), f32),
            dma(2), dma(nx), dma(ny), dma(ny), dma(nx), dma(2), dma(nz), dma(2), dma(nx), dma(ny),
        ],
        compiler_params=pltpu.CompilerParams(collective_id=1, has_side_effects=True),
        name="right",
    )(mom, grad, low, orth)


def factor_kernel(gram, left, orth, a, diag):
    f32 = jnp.float32
    rank = gram.shape[0]
    rows = left.shape[0]
    size = 128
    sub = lax.broadcasted_iota(jnp.int32, (8, size), 0)
    lane = lax.broadcasted_iota(jnp.int32, (8, size), 1)
    at_row = lax.broadcasted_iota(jnp.int32, (size, size), 0)
    at_col = lax.broadcasted_iota(jnp.int32, (size, size), 1)
    trace = jnp.zeros((size, size), f32)
    for b in range(rank // size):
        s = slice(b * size, (b + 1) * size)
        trace = trace + jnp.where(at_row == at_col, gram[s, s], 0.0)
    shift = ridge_scale * (jnp.sum(trace) / rank)
    a[:rank] = gram[...]
    for b in range(rank // size):
        s = slice(b * size, (b + 1) * size)
        a[s, s] = gram[s, s] + jnp.where(at_row == at_col, shift, 0.0)
    a[rank:] = left[...]

    def spread(v, l):
        return jnp.broadcast_to(v[:, l : l + 1], (8, size))

    def everywhere(v, i):
        return jnp.broadcast_to(v[i : i + 1, :], (8, size))

    def folded(v):
        return jnp.broadcast_to(jnp.sum(v, axis=0, keepdims=True), (8, size))

    def packed(lines):
        out = lines[0]
        for i in range(1, 8):
            out = jnp.where(sub == i, lines[i], out)
        return out

    def dot(x, y):
        return lax.dot_general(
            x, y, (((1,), (1,)), ((), ())), precision=lax.Precision.HIGHEST, preferred_element_type=f32
        )

    @pl.loop(0, rank // size)
    def _(block):
        off = pl.multiple_of(block * size, size)
        diag[0] = a[pl.ds(off, size), pl.ds(off, size)]
        upper, inverse = [], []
        for s in range(size // 8):
            base = 8 * s
            lines, other = [], []
            for i in range(8):
                line = jnp.broadcast_to(diag[0, base + i : base + i + 1, :], (8, size))
                unit = jnp.where(lane == base + i, 1.0, 0.0)
                if s:
                    acc_u = acc_w = None
                    for t in range(s):
                        factor = spread(upper[t], base + i)
                        u, w = factor * upper[t], factor * inverse[t]
                        acc_u = u if acc_u is None else acc_u + u
                        acc_w = w if acc_w is None else acc_w + w
                    line = line - folded(acc_u)
                    unit = unit - folded(acc_w)
                lines.append(line)
                other.append(unit)
            panel = packed(lines)
            cols = [spread(panel, base + j) for j in range(8)]
            d = [[everywhere(cols[j], i) if j >= i else None for j in range(8)] for i in range(8)]
            for j in range(8):
                scale = lax.rsqrt(d[j][j])
                lines[j] = lines[j] * scale
                other[j] = other[j] * scale
                u = [None] * 8
                for i in range(j + 1, 8):
                    u[i] = d[j][i] * scale
                for i in range(j + 1, 8):
                    for m in range(i, 8):
                        d[i][m] = d[i][m] - u[i] * u[m]
                for i in range(j + 1, 8):
                    lines[i] = lines[i] - u[i] * lines[j]
                    other[i] = other[i] - u[i] * other[j]
            upper.append(packed(lines))
            inverse.append(packed(other))
            diag[1, base : base + 8, :] = inverse[s]
        for b in range(rank // size):

            @pl.when(block == b)
            def _():
                at, after = b * size, (b + 1) * size
                below = dot(a[after:, at:after], diag[1])
                a[after:, at:after] = below
                if after < rank:
                    a[after:, after:] = a[after:, after:] - dot(below, below[: rank - after])

    orth[...] = a[rank:]


def factor_call(gram, left):
    rank, rows = gram.shape[0], left.shape[0]
    vmem = pl.BlockSpec(memory_space=pltpu.VMEM)
    return pl.pallas_call(
        factor_kernel,
        out_shape=jax.ShapeDtypeStruct((rows, rank), jnp.float32),
        in_specs=[vmem] * 2,
        out_specs=vmem,
        scratch_shapes=[pltpu.VMEM((rank + rows, rank), jnp.float32), pltpu.VMEM((2, 128, 128), jnp.float32)],
        name="factor",
    )(gram, left)


def per_device(gradients, momentum, right_basis):
    mom, grad = momentum[0], gradients[0]
    rank = right_basis.shape[1]
    whole_rows = mom.shape[0] * lax.axis_size(Y) * lax.axis_size(K)
    gram_matrix, left_factor, merged_low = left_call(mom, grad, right_basis)
    orthonormal = factor_call(gram_matrix, left_factor)
    new_momentum, new_basis, update = right_call(
        mom, grad, merged_low, orthonormal, math.sqrt(whole_rows / rank)
    )
    return new_momentum[None], new_basis, update


def solution(mesh):
    torus = Mesh(
        mesh.devices.reshape(mesh.shape["grp"], mesh.shape["row"] // 2, 2, mesh.shape["col"]),
        (X, Y, K, Z),
    )
    return jax.shard_map(
        per_device,
        mesh=torus,
        in_specs=(P(X, ROW, Z), P(X, ROW, Z), P(Z, None)),
        out_specs=(P(X, ROW, Z), P(Z, None), P(ROW, Z)),
        check_vma=False,
    )
```

```python
import functools
import math

import jax
import jax.numpy as jnp
from jax import lax
from jax.experimental import pallas as pl
from jax.experimental.pallas import tpu as pltpu
from jax.sharding import Mesh
from jax.sharding import PartitionSpec as P

MESH = pl.DeviceIdType.MESH
X, Y, K, Z = "grp", "row_0", "row_1", "col"
ROW = (Y, K)

momentum_decay = 0.9
ridge_scale = 0.0001
epsilon = 1e-06


def peer_of(axis, offset):
    return lax.rem(lax.axis_index(axis) + offset, lax.axis_size(axis))


def meet(axes):
    barrier = pltpu.get_barrier_semaphore()
    count = 0
    for axis in axes:
        for j in range(1, lax.axis_size(axis)):
            pl.semaphore_signal(barrier, inc=1, device_id={axis: peer_of(axis, j)}, device_id_type=MESH)
            count += 1
    return lambda: pl.semaphore_wait(barrier, count)


def send(src, dst, send_sem, recv_sem, axis, peer):
    copy = pltpu.make_async_remote_copy(
        src_ref=src, dst_ref=dst, send_sem=send_sem, recv_sem=recv_sem,
        device_id={axis: peer}, device_id_type=MESH,
    )
    copy.start()
    return copy


def scatter(tiles, arrived, sems, axis):
    copies = []
    for j in range(1, lax.axis_size(axis)):
        peer = peer_of(axis, j)
        copies.append(send(tiles.at[peer], arrived.at[j - 1], sems.at[0, j - 1], sems.at[1, j - 1], axis, peer))
    return copies


def share(slot, sems, axis):
    return [
        send(slot, slot, sems.at[0, j - 1], sems.at[1, j - 1], axis, peer_of(axis, j))
        for j in range(1, lax.axis_size(axis))
    ]


def arrive(copies):
    for copy in copies:
        copy.wait_recv()


def depart(copies):
    for copy in copies:
        copy.wait_send()


def left_kernel(
    mom, grad, basis, gram, left, low, part, xin, zpart, zin, lall, gall, gpair, kin, yall, gfull,
    sx, sz, sza, sxa, sk, sy, sgz, sgx, sgk,
):
    nx, ny, nz = lax.axis_size(X), lax.axis_size(Y), lax.axis_size(Z)
    g, y, k, c = (lax.axis_index(a) for a in (X, Y, K, Z))
    gathered = meet((X, Y, K, Z))
    chunks, lanes = part.shape[0], part.shape[3]
    tall = 4 * nz
    merged_low = (mom[...] + grad[...].astype(jnp.float32)).astype(jnp.bfloat16)
    low[...] = merged_low
    product = jnp.dot(merged_low, basis[...], preferred_element_type=jnp.float32)
    for t in range(chunks):
        for b in range(nx):
            part[t, b] = product[t * tall : (t + 1) * tall, b * lanes : (b + 1) * lanes]
    gathered()
    pending = []

    def started(copies):
        pending.extend(copies)
        return copies

    sent = [started(scatter(part.at[t], xin.at[t], sx.at[t], X)) for t in range(chunks)]
    after = []
    for t in range(chunks):
        arrive(sent[t])
        total = part[t, g]
        for j in range(nx - 1):
            total = total + xin[t, j]
        for q in range(nz):
            zpart[t, q] = total[4 * q : 4 * q + 4]
        after.append(started(scatter(zpart.at[t], zin.at[t], sz.at[t], Z)))
    sent, after = after, []
    for t in range(chunks):
        arrive(sent[t])
        own = zpart[t, c]
        for j in range(nz - 1):
            own = own + zin[t, j]
        lall[t, g, c] = own
        after.append(started(share(lall.at[t, g, c], sza.at[t], Z)))
    sent, after = after, []
    for t in range(chunks):
        arrive(sent[t])
        after.append(started(share(lall.at[t, g], sxa.at[t], X)))
    for t in range(chunks):
        arrive(after[t])
        rows = slice(t * tall, (t + 1) * tall)
        for b in range(nx):
            for q in range(nz):
                left[t * tall + 4 * q : t * tall + 4 * q + 4, b * lanes : (b + 1) * lanes] = lall[t, b, q]
        mine = left[rows, pl.ds(pl.multiple_of(g * lanes, lanes), lanes)]
        outer = lax.dot_general(
            mine, left[rows, :], (((0,), (0,)), ((), ())),
            precision=lax.Precision.HIGHEST, preferred_element_type=jnp.float32,
        )
        gall[...] = outer if t == 0 else gall[...] + outer
    strip = gall[pl.ds(pl.multiple_of(c * 8, 8), 8), :]
    half = strip.shape[1] // 2
    gpair[0] = strip[:, :half]
    gpair[1] = strip[:, half:]
    sent = started(scatter(gpair, kin, sk, K))
    arrive(sent)
    yall[y] = gpair[k] + kin[0]
    sent = started(share(yall.at[y], sy, Y))
    arrive(sent)
    total = yall[0]
    for j in range(1, ny):
        total = total + yall[j]
    parts = gfull.shape[1]
    wide = half // parts
    sent = []
    for u in range(parts):
        gfull[k, u, g, c] = total[:, u * wide : (u + 1) * wide]
        sent.append(started(share(gfull.at[k, u, g, c], sgz.at[u], Z)))
    after = []
    for u in range(parts):
        arrive(sent[u])
        after.append(started(share(gfull.at[k, u, g], sgx.at[u], X)))
    sent = []
    for u in range(parts):
        arrive(after[u])
        sent.append(started(share(gfull.at[k, u], sgk.at[u], K)))
    for u in range(parts):
        arrive(sent[u])
    for h in range(2):
        for u in range(parts):
            for b in range(nx):
                for q in range(nz):
                    at = (b * nz + q) * 8
                    lane = h * half + u * wide
                    gram[at : at + 8, lane : lane + wide] = gfull[h, u, b, q]
    depart(pending)


def copies_of(count, n):
    return pltpu.SemaphoreType.DMA((count, 2, n - 1) if count else (2, n - 1))


def left_call(mom, grad, basis):
    nx, ny, nz = lax.axis_size(X), lax.axis_size(Y), lax.axis_size(Z)
    rows, cols = mom.shape
    rank = basis.shape[1]
    lanes = rank // nx
    chunks = rows // (4 * nz)
    half = rank // 2
    f32 = jnp.float32
    vmem = pl.BlockSpec(memory_space=pltpu.VMEM)
    return pl.pallas_call(
        left_kernel,
        out_shape=(
            jax.ShapeDtypeStruct((rank, rank), f32),
            jax.ShapeDtypeStruct((rows, rank), f32),
            jax.ShapeDtypeStruct((rows, cols), jnp.bfloat16),
        ),
        in_specs=[vmem] * 3,
        out_specs=(vmem,) * 3,
        scratch_shapes=[
            pltpu.VMEM((chunks, nx, 4 * nz, lanes), f32),
            pltpu.VMEM((chunks, nx - 1, 4 * nz, lanes), f32),
            pltpu.VMEM((chunks, nz, 4, lanes), f32),
            pltpu.VMEM((chunks, nz - 1, 4, lanes), f32),
            pltpu.VMEM((chunks, nx, nz, 4, lanes), f32),
            pltpu.VMEM((lanes, rank), f32),
            pltpu.VMEM((2, 8, half), f32),
            pltpu.VMEM((1, 8, half), f32),
            pltpu.VMEM((ny, 8, half), f32),
            pltpu.VMEM((2, 2, nx, nz, 8, half // 2), f32),
            copies_of(chunks, nx), copies_of(chunks, nz), copies_of(chunks, nz), copies_of(chunks, nx),
            copies_of(0, 2), copies_of(0, ny), copies_of(2, nz), copies_of(2, nx), copies_of(2, 2),
        ],
        compiler_params=pltpu.CompilerParams(collective_id=0, has_side_effects=True),
        name="left",
    )(mom, grad, basis)


def right_kernel(
    groups, whole_rows, low, orth, nb_out, rms_out, ksend, kin, mine, xsend, xin, ysum, ysend, yin, nb, low_left,
    qz, qk, qx, qy, sk, sx, sy, say, sax, sak, sqz, sqk, sqx, sqy,
):
    nx, ny, nz = lax.axis_size(X), lax.axis_size(Y), lax.axis_size(Z)
    g, y, k, c = (lax.axis_index(a) for a in (X, Y, K, Z))
    gathered = meet((X, Y, K, Z))
    chunks, half, wide = ksend.shape
    f32, bf16 = jnp.float32, jnp.bfloat16
    low_left[...] = orth[...].astype(bf16)
    pending = []

    def started(copies):
        pending.extend(copies)
        return copies

    def product(at):
        return lax.dot_general(
            low[:, pl.ds(pl.multiple_of(at, 128), 128)], low_left[...], (((0,), (0,)), ((), ())),
            preferred_element_type=f32,
        ) * (1.0 / groups)

    @pl.loop(0, half // 128)
    def _(i):
        tile = product((1 - k) * half + i * 128).astype(bf16)
        for t in range(chunks):
            ksend[t, pl.ds(pl.multiple_of(i * 128, 128), 128), :] = tile[:, t * wide : (t + 1) * wide]

    gathered()
    sent = [
        started([send(ksend.at[t], kin.at[t], sk.at[t, 0, 0], sk.at[t, 1, 0], K, 1 - k)]) for t in range(chunks)
    ]

    @pl.loop(0, half // 128)
    def _(i):
        tile = product(k * half + i * 128)
        for t in range(chunks):
            mine[t, pl.ds(pl.multiple_of(i * 128, 128), 128), :] = tile[:, t * wide : (t + 1) * wide]

    block = half // nx
    piece_rows = block // ny
    after = []
    for t in range(chunks):
        arrive(sent[t])
        for b in range(nx):
            at = slice(b * block, (b + 1) * block)
            both = mine[t, at] + kin[t, at].astype(f32)
            mine[t, at] = both
            xsend[t, b] = both.astype(bf16)
        after.append(started(scatter(xsend.at[t], xin.at[t], sx.at[t], X)))
    sent, after = after, []
    for t in range(chunks):
        arrive(sent[t])
        total = mine[t, pl.ds(pl.multiple_of(g * block, block), block), :]
        for j in range(nx - 1):
            total = total + xin[t, j].astype(f32)
        ysum[t] = total
        for b in range(ny):
            ysend[t, b] = total[b * piece_rows : (b + 1) * piece_rows].astype(bf16)
        after.append(started(scatter(ysend.at[t], yin.at[t], sy.at[t], Y)))
    sent, after = after, []
    for t in range(chunks):
        arrive(sent[t])
        piece = ysum[t, pl.ds(pl.multiple_of(y * piece_rows, 8), piece_rows), :]
        for j in range(ny - 1):
            piece = piece + yin[t, j].astype(f32)
        nb[t, k, g, y] = piece.astype(bf16)
        qz[c, :, t * wide : (t + 1) * wide] = jnp.sum(piece * piece, axis=0, keepdims=True)
        if t == chunks - 1:
            sent_q = started(share(qz.at[c], sqz, Z))
        after.append(started(share(nb.at[t, k, g, y], say.at[t], Y)))

    def summed(ref, n):
        acc = ref[0]
        for j in range(1, n):
            acc = acc + ref[j]
        return acc

    sent, after = after, []
    for t in range(chunks):
        arrive(sent[t])
        after.append(started(share(nb.at[t, k, g], sax.at[t], X)))
    arrive(sent_q)
    qy[y] = summed(qz, nz)
    sent_q = started(share(qy.at[y], sqy, Y))
    sent = []
    for t in range(chunks - 1):
        arrive(after[t])
        sent.append(started(share(nb.at[t, k], sak.at[t], K)))
    arrive(sent_q)
    qx[g] = summed(qy, ny)
    sent_q = started(share(qx.at[g], sqx, X))
    arrive(after[-1])
    sent.append(started(share(nb.at[chunks - 1, k], sak.at[chunks - 1], K)))
    arrive(sent_q)
    qk[k] = summed(qx, nx)
    sent_q = started(share(qk.at[k], sqk, K))
    for t in range(chunks):
        arrive(sent[t])
        for h in range(2):
            for b in range(nx):
                for p in range(ny):
                    at = h * half + b * block + p * piece_rows
                    nb_out[t, at : at + piece_rows, :] = nb[t, h, b, p]
    arrive(sent_q)
    rms_out[...] = jnp.sqrt(summed(qk, 2) / whole_rows + epsilon)
    depart(pending)


def right_call(low, orth):
    nx, ny, nz = lax.axis_size(X), lax.axis_size(Y), lax.axis_size(Z)
    rows, cols = low.shape
    rank = orth.shape[1]
    half = cols // 2
    block = half // nx
    piece = block // ny
    wide = 128
    chunks = rank // wide
    f32, bf16 = jnp.float32, jnp.bfloat16
    vmem = pl.BlockSpec(memory_space=pltpu.VMEM)
    return pl.pallas_call(
        functools.partial(right_kernel, nx, cols * nz),
        out_shape=(
            jax.ShapeDtypeStruct((chunks, cols, wide), bf16),
            jax.ShapeDtypeStruct((1, rank), f32),
        ),
        in_specs=[vmem] * 2,
        out_specs=(vmem,) * 2,
        scratch_shapes=[
            pltpu.VMEM((chunks, half, wide), bf16),
            pltpu.VMEM((chunks, half, wide), bf16),
            pltpu.VMEM((chunks, half, wide), f32),
            pltpu.VMEM((chunks, nx, block, wide), bf16),
            pltpu.VMEM((chunks, nx - 1, block, wide), bf16),
            pltpu.VMEM((chunks, block, wide), f32),
            pltpu.VMEM((chunks, ny, piece, wide), bf16),
            pltpu.VMEM((chunks, ny - 1, piece, wide), bf16),
            pltpu.VMEM((chunks, 2, nx, ny, piece, wide), bf16),
            pltpu.VMEM((rows, rank), bf16),
            pltpu.VMEM((nz, 1, rank), f32),
            pltpu.VMEM((2, 1, rank), f32),
            pltpu.VMEM((nx, 1, rank), f32),
            pltpu.VMEM((ny, 1, rank), f32),
            copies_of(chunks, 2), copies_of(chunks, nx), copies_of(chunks, ny), copies_of(chunks, ny),
            copies_of(chunks, nx), copies_of(chunks, 2),
            copies_of(0, nz), copies_of(0, 2), copies_of(0, nx), copies_of(0, ny),
        ],
        compiler_params=pltpu.CompilerParams(collective_id=1, has_side_effects=True),
        name="right",
    )(low, orth)


def final_kernel(update_scale, nb, rms, orth, mom, grad, newmom, basis, update, stack):
    rows = mom.shape[0]
    chunks, wide = nb.shape[0], nb.shape[2]
    f32, bf16 = jnp.float32, jnp.bfloat16

    @pl.when(pl.program_id(0) == 0)
    def _():
        stack[:rows] = orth[...].astype(bf16)
        stack[rows:] = (orth[...] * rms[...]).astype(bf16)

    inverse = 1.0 / rms[...]
    for t in range(chunks):
        at = slice(t * wide, (t + 1) * wide)
        basis[:, at] = (nb[t].astype(f32) * inverse[:, at]).astype(bf16)
    both = lax.dot_general(stack[...], basis[...], (((1,), (1,)), ((), ())), preferred_element_type=f32)
    update[...] = (update_scale * both[:rows]).astype(bf16)
    newmom[...] = mom[...] + grad[...].astype(f32) - (1 - momentum_decay) * both[rows:]


def final_call(nb, rms, orth, mom, grad, update_scale):
    chunks, cols, wide = nb.shape
    rows, rank = orth.shape
    step = 512
    f32, bf16 = jnp.float32, jnp.bfloat16
    strip = pl.BlockSpec((rows, step), lambda i: (0, i))
    return pl.pallas_call(
        functools.partial(final_kernel, update_scale),
        grid=(cols // step,),
        out_shape=(
            jax.ShapeDtypeStruct((rows, cols), f32),
            jax.ShapeDtypeStruct((cols, rank), bf16),
            jax.ShapeDtypeStruct((rows, cols), bf16),
        ),
        in_specs=[
            pl.BlockSpec((chunks, step, wide), lambda i: (0, i, 0)),
            pl.BlockSpec((1, rank), lambda i: (0, 0)),
            pl.BlockSpec((rows, rank), lambda i: (0, 0)),
            strip,
            strip,
        ],
        out_specs=(strip, pl.BlockSpec((step, rank), lambda i: (i, 0)), strip),
        scratch_shapes=[pltpu.VMEM((2 * rows, rank), bf16)],
        name="final",
    )(nb, rms, orth, mom, grad)


def factor_kernel(gram, left, orth, a, diag):
    f32 = jnp.float32
    rank = gram.shape[0]
    rows = left.shape[0]
    size = 128
    sub = lax.broadcasted_iota(jnp.int32, (8, size), 0)
    lane = lax.broadcasted_iota(jnp.int32, (8, size), 1)
    at_row = lax.broadcasted_iota(jnp.int32, (size, size), 0)
    at_col = lax.broadcasted_iota(jnp.int32, (size, size), 1)
    trace = jnp.zeros((size, size), f32)
    for b in range(rank // size):
        s = slice(b * size, (b + 1) * size)
        trace = trace + jnp.where(at_row == at_col, gram[s, s], 0.0)
    shift = ridge_scale * (jnp.sum(trace) / rank)
    a[:rank] = gram[...]
    for b in range(rank // size):
        s = slice(b * size, (b + 1) * size)
        a[s, s] = gram[s, s] + jnp.where(at_row == at_col, shift, 0.0)
    a[rank:] = left[...]

    def spread(v, l):
        return jnp.broadcast_to(v[:, l : l + 1], (8, size))

    def everywhere(v, i):
        return jnp.broadcast_to(v[i : i + 1, :], (8, size))

    def folded(v):
        return jnp.broadcast_to(jnp.sum(v, axis=0, keepdims=True), (8, size))

    def packed(lines):
        out = lines[0]
        for i in range(1, 8):
            out = jnp.where(sub == i, lines[i], out)
        return out

    def dot(x, y):
        return lax.dot_general(
            x, y, (((1,), (1,)), ((), ())), precision=lax.Precision.HIGHEST, preferred_element_type=f32
        )

    @pl.loop(0, rank // size)
    def _(block):
        off = pl.multiple_of(block * size, size)
        diag[0] = a[pl.ds(off, size), pl.ds(off, size)]
        upper, inverse = [], []
        for s in range(size // 8):
            base = 8 * s
            lines, other = [], []
            for i in range(8):
                line = jnp.broadcast_to(diag[0, base + i : base + i + 1, :], (8, size))
                unit = jnp.where(lane == base + i, 1.0, 0.0)
                if s:
                    acc_u = acc_w = None
                    for t in range(s):
                        factor = spread(upper[t], base + i)
                        u, w = factor * upper[t], factor * inverse[t]
                        acc_u = u if acc_u is None else acc_u + u
                        acc_w = w if acc_w is None else acc_w + w
                    line = line - folded(acc_u)
                    unit = unit - folded(acc_w)
                lines.append(line)
                other.append(unit)
            panel = packed(lines)
            cols = [spread(panel, base + j) for j in range(8)]
            d = [[everywhere(cols[j], i) if j >= i else None for j in range(8)] for i in range(8)]
            for j in range(8):
                scale = lax.rsqrt(d[j][j])
                lines[j] = lines[j] * scale
                other[j] = other[j] * scale
                u = [None] * 8
                for i in range(j + 1, 8):
                    u[i] = d[j][i] * scale
                for i in range(j + 1, 8):
                    for m in range(i, 8):
                        d[i][m] = d[i][m] - u[i] * u[m]
                for i in range(j + 1, 8):
                    lines[i] = lines[i] - u[i] * lines[j]
                    other[i] = other[i] - u[i] * other[j]
            upper.append(packed(lines))
            inverse.append(packed(other))
            diag[1, base : base + 8, :] = inverse[s]
        for b in range(rank // size):

            @pl.when(block == b)
            def _():
                at, after = b * size, (b + 1) * size
                below = dot(a[after:, at:after], diag[1])
                a[after:, at:after] = below
                if after < rank:
                    a[after:, after:] = a[after:, after:] - dot(below, below[: rank - after])

    orth[...] = a[rank:]


def factor_call(gram, left):
    rank, rows = gram.shape[0], left.shape[0]
    vmem = pl.BlockSpec(memory_space=pltpu.VMEM)
    return pl.pallas_call(
        factor_kernel,
        out_shape=jax.ShapeDtypeStruct((rows, rank), jnp.float32),
        in_specs=[vmem] * 2,
        out_specs=vmem,
        scratch_shapes=[pltpu.VMEM((rank + rows, rank), jnp.float32), pltpu.VMEM((2, 128, 128), jnp.float32)],
        name="factor",
    )(gram, left)


def per_device(gradients, momentum, right_basis):
    mom, grad = momentum[0], gradients[0]
    rank = right_basis.shape[1]
    whole_rows = mom.shape[0] * lax.axis_size(Y) * lax.axis_size(K)
    gram_matrix, left_factor, merged_low = left_call(mom, grad, right_basis)
    orthonormal = factor_call(gram_matrix, left_factor)
    gathered, column_rms = right_call(merged_low, orthonormal)
    new_momentum, new_basis, update = final_call(
        gathered, column_rms, orthonormal, mom, grad, math.sqrt(whole_rows / rank)
    )
    return new_momentum[None], new_basis, update


def solution(mesh):
    torus = Mesh(
        mesh.devices.reshape(mesh.shape["grp"], mesh.shape["row"] // 2, 2, mesh.shape["col"]),
        (X, Y, K, Z),
    )
    return jax.shard_map(
        per_device,
        mesh=torus,
        in_specs=(P(X, ROW, Z), P(X, ROW, Z), P(Z, None)),
        out_specs=(P(X, ROW, Z), P(Z, None), P(ROW, Z)),
        check_vma=False,
    )
```

```python
import functools
import math

import jax
import jax.numpy as jnp
from jax import lax
from jax.experimental import pallas as pl
from jax.experimental.pallas import tpu as pltpu
from jax.sharding import Mesh
from jax.sharding import PartitionSpec as P

MESH = pl.DeviceIdType.MESH
X, Y, K, Z = "grp", "row_0", "row_1", "col"
ROW = (Y, K)

momentum_decay = 0.9
ridge_scale = 0.0001
epsilon = 1e-06


def peer_of(axis, offset):
    return lax.rem(lax.axis_index(axis) + offset, lax.axis_size(axis))


def meet(axes):
    barrier = pltpu.get_barrier_semaphore()
    count = 0
    for axis in axes:
        for j in range(1, lax.axis_size(axis)):
            pl.semaphore_signal(barrier, inc=1, device_id={axis: peer_of(axis, j)}, device_id_type=MESH)
            count += 1
    return lambda: pl.semaphore_wait(barrier, count)


def send(src, dst, send_sem, recv_sem, axis, peer):
    copy = pltpu.make_async_remote_copy(
        src_ref=src, dst_ref=dst, send_sem=send_sem, recv_sem=recv_sem,
        device_id={axis: peer}, device_id_type=MESH,
    )
    copy.start()
    return copy


def scatter(tiles, arrived, sems, axis):
    copies = []
    for j in range(1, lax.axis_size(axis)):
        peer = peer_of(axis, j)
        copies.append(send(tiles.at[peer], arrived.at[j - 1], sems.at[0, j - 1], sems.at[1, j - 1], axis, peer))
    return copies


def share(slot, sems, axis):
    return [
        send(slot, slot, sems.at[0, j - 1], sems.at[1, j - 1], axis, peer_of(axis, j))
        for j in range(1, lax.axis_size(axis))
    ]


def arrive(copies):
    for copy in copies:
        copy.wait_recv()


def depart(copies):
    for copy in copies:
        copy.wait_send()


def left_kernel(
    mom, grad, basis, gram, left, low, part, xin, zpart, zin, lall, gall, gpair, kin, gy, gyin, gfull,
    sx, sz, sza, sxa, sk, sy, sgy, sgx, sgk,
):
    nx, ny, nz = lax.axis_size(X), lax.axis_size(Y), lax.axis_size(Z)
    g, y, k, c = (lax.axis_index(a) for a in (X, Y, K, Z))
    gathered = meet((X, Y, K, Z))
    chunks, lanes = part.shape[0], part.shape[3]
    tall = 4 * nz
    merged_low = (mom[...] + grad[...].astype(jnp.float32)).astype(jnp.bfloat16)
    low[...] = merged_low
    product = jnp.dot(merged_low, basis[...], preferred_element_type=jnp.float32)
    for t in range(chunks):
        for b in range(nx):
            part[t, b] = product[t * tall : (t + 1) * tall, b * lanes : (b + 1) * lanes]
    gathered()
    pending = []

    def started(copies):
        pending.extend(copies)
        return copies

    sent = [started(scatter(part.at[t], xin.at[t], sx.at[t], X)) for t in range(chunks)]
    after = []
    for t in range(chunks):
        arrive(sent[t])
        total = part[t, g]
        for j in range(nx - 1):
            total = total + xin[t, j]
        for q in range(nz):
            zpart[t, q] = total[4 * q : 4 * q + 4]
        after.append(started(scatter(zpart.at[t], zin.at[t], sz.at[t], Z)))
    sent, after = after, []
    for t in range(chunks):
        arrive(sent[t])
        own = zpart[t, c]
        for j in range(nz - 1):
            own = own + zin[t, j]
        lall[t, g, c] = own
        after.append(started(share(lall.at[t, g, c], sza.at[t], Z)))
    sent, after = after, []
    for t in range(chunks):
        arrive(sent[t])
        after.append(started(share(lall.at[t, g], sxa.at[t], X)))
    for t in range(chunks):
        arrive(after[t])
        rows = slice(t * tall, (t + 1) * tall)
        for b in range(nx):
            for q in range(nz):
                left[t * tall + 4 * q : t * tall + 4 * q + 4, b * lanes : (b + 1) * lanes] = lall[t, b, q]
        mine = left[rows, pl.ds(pl.multiple_of(g * lanes, lanes), lanes)]
        outer = lax.dot_general(
            mine, left[rows, :], (((0,), (0,)), ((), ())),
            precision=lax.Precision.HIGHEST, preferred_element_type=jnp.float32,
        )
        gall[...] = outer if t == 0 else gall[...] + outer
    half = gall.shape[1] // 2
    parts, wide = gpair.shape[0], gpair.shape[3]
    deep = lanes // ny
    sent = []
    for u in range(parts):
        for h in range(2):
            lane = h * half + u * wide
            gpair[u, h] = gall[:, lane : lane + wide]
        sent.append(started(scatter(gpair.at[u], kin.at[u], sk.at[u], K)))
    after = []
    for u in range(parts):
        arrive(sent[u])
        total = gpair[u, k] + kin[u, 0]
        for p in range(ny):
            gy[u, p] = total[p * deep : (p + 1) * deep]
        after.append(started(scatter(gy.at[u], gyin.at[u], sy.at[u], Y)))
    sent, after = after, []
    for u in range(parts):
        arrive(sent[u])
        own = gy[u, y]
        for j in range(ny - 1):
            own = own + gyin[u, j]
        gfull[k, u, g, y] = own
        after.append(started(share(gfull.at[k, u, g, y], sgy.at[u], Y)))
    sent, after = after, []
    for u in range(parts):
        arrive(sent[u])
        after.append(started(share(gfull.at[k, u, g], sgx.at[u], X)))
    sent = []
    for u in range(parts):
        arrive(after[u])
        sent.append(started(share(gfull.at[k, u], sgk.at[u], K)))
    for u in range(parts):
        arrive(sent[u])
        for h in range(2):
            for b in range(nx):
                for p in range(ny):
                    at = b * lanes + p * deep
                    lane = h * half + u * wide
                    gram[at : at + deep, lane : lane + wide] = gfull[h, u, b, p]
    depart(pending)


def copies_of(count, n):
    return pltpu.SemaphoreType.DMA((count, 2, n - 1) if count else (2, n - 1))


def left_call(mom, grad, basis):
    nx, ny, nz = lax.axis_size(X), lax.axis_size(Y), lax.axis_size(Z)
    rows, cols = mom.shape
    rank = basis.shape[1]
    lanes = rank // nx
    chunks = rows // (4 * nz)
    half = rank // 2
    f32 = jnp.float32
    vmem = pl.BlockSpec(memory_space=pltpu.VMEM)
    return pl.pallas_call(
        left_kernel,
        out_shape=(
            jax.ShapeDtypeStruct((rank, rank), f32),
            jax.ShapeDtypeStruct((rows, rank), f32),
            jax.ShapeDtypeStruct((rows, cols), jnp.bfloat16),
        ),
        in_specs=[vmem] * 3,
        out_specs=(vmem,) * 3,
        scratch_shapes=[
            pltpu.VMEM((chunks, nx, 4 * nz, lanes), f32),
            pltpu.VMEM((chunks, nx - 1, 4 * nz, lanes), f32),
            pltpu.VMEM((chunks, nz, 4, lanes), f32),
            pltpu.VMEM((chunks, nz - 1, 4, lanes), f32),
            pltpu.VMEM((chunks, nx, nz, 4, lanes), f32),
            pltpu.VMEM((lanes, rank), f32),
            pltpu.VMEM((2, 2, lanes, half // 2), f32),
            pltpu.VMEM((2, 1, lanes, half // 2), f32),
            pltpu.VMEM((2, ny, lanes // ny, half // 2), f32),
            pltpu.VMEM((2, ny - 1, lanes // ny, half // 2), f32),
            pltpu.VMEM((2, 2, nx, ny, lanes // ny, half // 2), f32),
            copies_of(chunks, nx), copies_of(chunks, nz), copies_of(chunks, nz), copies_of(chunks, nx),
            copies_of(2, 2), copies_of(2, ny), copies_of(2, ny), copies_of(2, nx), copies_of(2, 2),
        ],
        compiler_params=pltpu.CompilerParams(collective_id=0, has_side_effects=True, vmem_limit_bytes=24 << 20),
        name="left",
    )(mom, grad, basis)


def right_kernel(
    groups, whole_rows, low, orth, nb_out, rms_out, ksend, kin, mine, xsend, xin, ysum, ysend, yin, nb, low_left,
    qz, qk, qx, qy, sk, sx, sy, say, sax, sak, sqz, sqk, sqx, sqy,
):
    nx, ny, nz = lax.axis_size(X), lax.axis_size(Y), lax.axis_size(Z)
    g, y, k, c = (lax.axis_index(a) for a in (X, Y, K, Z))
    gathered = meet((X, Y, K, Z))
    chunks, half, wide = ksend.shape
    f32, bf16 = jnp.float32, jnp.bfloat16
    low_left[...] = orth[...].astype(bf16)
    pending = []

    def started(copies):
        pending.extend(copies)
        return copies

    def product(at):
        return lax.dot_general(
            low[:, pl.ds(pl.multiple_of(at, 128), 128)], low_left[...], (((0,), (0,)), ((), ())),
            preferred_element_type=f32,
        ) * (1.0 / groups)

    @pl.loop(0, half // 128)
    def _(i):
        tile = product((1 - k) * half + i * 128).astype(bf16)
        for t in range(chunks):
            ksend[t, pl.ds(pl.multiple_of(i * 128, 128), 128), :] = tile[:, t * wide : (t + 1) * wide]

    gathered()
    sent = [
        started([send(ksend.at[t], kin.at[t], sk.at[t, 0, 0], sk.at[t, 1, 0], K, 1 - k)]) for t in range(chunks)
    ]

    @pl.loop(0, half // 128)
    def _(i):
        tile = product(k * half + i * 128)
        for t in range(chunks):
            mine[t, pl.ds(pl.multiple_of(i * 128, 128), 128), :] = tile[:, t * wide : (t + 1) * wide]

    block = half // nx
    piece_rows = block // ny
    after = []
    for t in range(chunks):
        arrive(sent[t])
        for b in range(nx):
            at = slice(b * block, (b + 1) * block)
            both = mine[t, at] + kin[t, at].astype(f32)
            mine[t, at] = both
            xsend[t, b] = both.astype(bf16)
        after.append(started(scatter(xsend.at[t], xin.at[t], sx.at[t], X)))
    sent, after = after, []
    for t in range(chunks):
        arrive(sent[t])
        total = mine[t, pl.ds(pl.multiple_of(g * block, block), block), :]
        for j in range(nx - 1):
            total = total + xin[t, j].astype(f32)
        ysum[t] = total
        for b in range(ny):
            ysend[t, b] = total[b * piece_rows : (b + 1) * piece_rows].astype(bf16)
        after.append(started(scatter(ysend.at[t], yin.at[t], sy.at[t], Y)))
    sent, after = after, []
    for t in range(chunks):
        arrive(sent[t])
        piece = ysum[t, pl.ds(pl.multiple_of(y * piece_rows, 8), piece_rows), :]
        for j in range(ny - 1):
            piece = piece + yin[t, j].astype(f32)
        nb[t, k, g, y] = piece.astype(bf16)
        qz[c, :, t * wide : (t + 1) * wide] = jnp.sum(piece * piece, axis=0, keepdims=True)
        if t == chunks - 1:
            sent_q = started(share(qz.at[c], sqz, Z))
        after.append(started(share(nb.at[t, k, g, y], say.at[t], Y)))

    def summed(ref, n):
        acc = ref[0]
        for j in range(1, n):
            acc = acc + ref[j]
        return acc

    sent, after = after, []
    for t in range(chunks):
        arrive(sent[t])
        after.append(started(share(nb.at[t, k, g], sax.at[t], X)))
    arrive(sent_q)
    qy[y] = summed(qz, nz)
    sent_q = started(share(qy.at[y], sqy, Y))
    sent = []
    for t in range(chunks - 1):
        arrive(after[t])
        sent.append(started(share(nb.at[t, k], sak.at[t], K)))
    arrive(sent_q)
    qx[g] = summed(qy, ny)
    sent_q = started(share(qx.at[g], sqx, X))
    arrive(after[-1])
    sent.append(started(share(nb.at[chunks - 1, k], sak.at[chunks - 1], K)))
    arrive(sent_q)
    qk[k] = summed(qx, nx)
    sent_q = started(share(qk.at[k], sqk, K))
    for t in range(chunks):
        arrive(sent[t])
        for h in range(2):
            for b in range(nx):
                for p in range(ny):
                    at = h * half + b * block + p * piece_rows
                    nb_out[t, at : at + piece_rows, :] = nb[t, h, b, p]
    arrive(sent_q)
    rms_out[...] = jnp.sqrt(summed(qk, 2) / whole_rows + epsilon)
    depart(pending)


def right_call(low, orth):
    nx, ny, nz = lax.axis_size(X), lax.axis_size(Y), lax.axis_size(Z)
    rows, cols = low.shape
    rank = orth.shape[1]
    half = cols // 2
    block = half // nx
    piece = block // ny
    wide = 128
    chunks = rank // wide
    f32, bf16 = jnp.float32, jnp.bfloat16
    vmem = pl.BlockSpec(memory_space=pltpu.VMEM)
    return pl.pallas_call(
        functools.partial(right_kernel, nx, cols * nz),
        out_shape=(
            jax.ShapeDtypeStruct((chunks, cols, wide), bf16),
            jax.ShapeDtypeStruct((1, rank), f32),
        ),
        in_specs=[vmem] * 2,
        out_specs=(vmem,) * 2,
        scratch_shapes=[
            pltpu.VMEM((chunks, half, wide), bf16),
            pltpu.VMEM((chunks, half, wide), bf16),
            pltpu.VMEM((chunks, half, wide), f32),
            pltpu.VMEM((chunks, nx, block, wide), bf16),
            pltpu.VMEM((chunks, nx - 1, block, wide), bf16),
            pltpu.VMEM((chunks, block, wide), f32),
            pltpu.VMEM((chunks, ny, piece, wide), bf16),
            pltpu.VMEM((chunks, ny - 1, piece, wide), bf16),
            pltpu.VMEM((chunks, 2, nx, ny, piece, wide), bf16),
            pltpu.VMEM((rows, rank), bf16),
            pltpu.VMEM((nz, 1, rank), f32),
            pltpu.VMEM((2, 1, rank), f32),
            pltpu.VMEM((nx, 1, rank), f32),
            pltpu.VMEM((ny, 1, rank), f32),
            copies_of(chunks, 2), copies_of(chunks, nx), copies_of(chunks, ny), copies_of(chunks, ny),
            copies_of(chunks, nx), copies_of(chunks, 2),
            copies_of(0, nz), copies_of(0, 2), copies_of(0, nx), copies_of(0, ny),
        ],
        compiler_params=pltpu.CompilerParams(collective_id=1, has_side_effects=True, vmem_limit_bytes=24 << 20),
        name="right",
    )(low, orth)


def final_kernel(update_scale, nb, rms, orth, mom, grad, newmom, basis, update, stack):
    rows = mom.shape[0]
    chunks, wide = nb.shape[0], nb.shape[2]
    f32, bf16 = jnp.float32, jnp.bfloat16

    @pl.when(pl.program_id(0) == 0)
    def _():
        stack[:rows] = orth[...].astype(bf16)
        stack[rows:] = (orth[...] * rms[...]).astype(bf16)

    inverse = 1.0 / rms[...]
    for t in range(chunks):
        at = slice(t * wide, (t + 1) * wide)
        basis[:, at] = (nb[t].astype(f32) * inverse[:, at]).astype(bf16)
    both = lax.dot_general(stack[...], basis[...], (((1,), (1,)), ((), ())), preferred_element_type=f32)
    update[...] = (update_scale * both[:rows]).astype(bf16)
    newmom[...] = mom[...] + grad[...].astype(f32) - (1 - momentum_decay) * both[rows:]


def final_call(nb, rms, orth, mom, grad, update_scale):
    chunks, cols, wide = nb.shape
    rows, rank = orth.shape
    step = 512
    f32, bf16 = jnp.float32, jnp.bfloat16
    strip = pl.BlockSpec((rows, step), lambda i: (0, i))
    return pl.pallas_call(
        functools.partial(final_kernel, update_scale),
        grid=(cols // step,),
        out_shape=(
            jax.ShapeDtypeStruct((rows, cols), f32),
            jax.ShapeDtypeStruct((cols, rank), bf16),
            jax.ShapeDtypeStruct((rows, cols), bf16),
        ),
        in_specs=[
            pl.BlockSpec((chunks, step, wide), lambda i: (0, i, 0)),
            pl.BlockSpec((1, rank), lambda i: (0, 0)),
            pl.BlockSpec((rows, rank), lambda i: (0, 0)),
            strip,
            strip,
        ],
        out_specs=(strip, pl.BlockSpec((step, rank), lambda i: (i, 0)), strip),
        scratch_shapes=[pltpu.VMEM((2 * rows, rank), bf16)],
        compiler_params=pltpu.CompilerParams(vmem_limit_bytes=16 << 20),
        name="final",
    )(nb, rms, orth, mom, grad)


def factor_kernel(gram, left, orth, a, diag):
    f32 = jnp.float32
    rank = gram.shape[0]
    rows = left.shape[0]
    size = 128
    sub = lax.broadcasted_iota(jnp.int32, (8, size), 0)
    lane = lax.broadcasted_iota(jnp.int32, (8, size), 1)
    at_row = lax.broadcasted_iota(jnp.int32, (size, size), 0)
    at_col = lax.broadcasted_iota(jnp.int32, (size, size), 1)
    trace = jnp.zeros((size, size), f32)
    for b in range(rank // size):
        s = slice(b * size, (b + 1) * size)
        trace = trace + jnp.where(at_row == at_col, gram[s, s], 0.0)
    shift = ridge_scale * (jnp.sum(trace) / rank)
    a[:rank] = gram[...]
    for b in range(rank // size):
        s = slice(b * size, (b + 1) * size)
        a[s, s] = gram[s, s] + jnp.where(at_row == at_col, shift, 0.0)
    a[rank:] = left[...]

    def spread(v, l):
        return jnp.broadcast_to(v[:, l : l + 1], (8, size))

    def everywhere(v, i):
        return jnp.broadcast_to(v[i : i + 1, :], (8, size))

    def folded(v):
        return jnp.broadcast_to(jnp.sum(v, axis=0, keepdims=True), (8, size))

    def packed(lines):
        out = lines[0]
        for i in range(1, 8):
            out = jnp.where(sub == i, lines[i], out)
        return out

    def dot(x, y):
        return lax.dot_general(
            x, y, (((1,), (1,)), ((), ())), precision=lax.Precision.HIGHEST, preferred_element_type=f32
        )

    @pl.loop(0, rank // size)
    def _(block):
        off = pl.multiple_of(block * size, size)
        diag[0] = a[pl.ds(off, size), pl.ds(off, size)]
        upper, inverse = [], []
        for s in range(size // 8):
            base = 8 * s
            lines, other = [], []
            for i in range(8):
                line = jnp.broadcast_to(diag[0, base + i : base + i + 1, :], (8, size))
                unit = jnp.where(lane == base + i, 1.0, 0.0)
                if s:
                    acc_u = acc_w = None
                    for t in range(s):
                        factor = spread(upper[t], base + i)
                        u, w = factor * upper[t], factor * inverse[t]
                        acc_u = u if acc_u is None else acc_u + u
                        acc_w = w if acc_w is None else acc_w + w
                    line = line - folded(acc_u)
                    unit = unit - folded(acc_w)
                lines.append(line)
                other.append(unit)
            panel = packed(lines)
            cols = [spread(panel, base + j) for j in range(8)]
            d = [[everywhere(cols[j], i) if j >= i else None for j in range(8)] for i in range(8)]
            for j in range(8):
                scale = lax.rsqrt(d[j][j])
                lines[j] = lines[j] * scale
                other[j] = other[j] * scale
                u = [None] * 8
                for i in range(j + 1, 8):
                    u[i] = d[j][i] * scale
                for i in range(j + 1, 8):
                    for m in range(i, 8):
                        d[i][m] = d[i][m] - u[i] * u[m]
                for i in range(j + 1, 8):
                    lines[i] = lines[i] - u[i] * lines[j]
                    other[i] = other[i] - u[i] * other[j]
            upper.append(packed(lines))
            inverse.append(packed(other))
            diag[1, base : base + 8, :] = inverse[s]
        for b in range(rank // size):

            @pl.when(block == b)
            def _():
                at, after = b * size, (b + 1) * size
                below = dot(a[after:, at:after], diag[1])
                a[after:, at:after] = below
                if after < rank:
                    a[after:, after:] = a[after:, after:] - dot(below, below[: rank - after])

    orth[...] = a[rank:]


def factor_call(gram, left):
    rank, rows = gram.shape[0], left.shape[0]
    vmem = pl.BlockSpec(memory_space=pltpu.VMEM)
    return pl.pallas_call(
        factor_kernel,
        out_shape=jax.ShapeDtypeStruct((rows, rank), jnp.float32),
        in_specs=[vmem] * 2,
        out_specs=vmem,
        scratch_shapes=[pltpu.VMEM((rank + rows, rank), jnp.float32), pltpu.VMEM((2, 128, 128), jnp.float32)],
        compiler_params=pltpu.CompilerParams(vmem_limit_bytes=16 << 20),
        name="factor",
    )(gram, left)


def per_device(gradients, momentum, right_basis):
    mom, grad = momentum[0], gradients[0]
    rank = right_basis.shape[1]
    whole_rows = mom.shape[0] * lax.axis_size(Y) * lax.axis_size(K)
    gram_matrix, left_factor, merged_low = left_call(mom, grad, right_basis)
    orthonormal = factor_call(gram_matrix, left_factor)
    gathered, column_rms = right_call(merged_low, orthonormal)
    new_momentum, new_basis, update = final_call(
        gathered, column_rms, orthonormal, mom, grad, math.sqrt(whole_rows / rank)
    )
    return new_momentum[None], new_basis, update


def solution(mesh):
    torus = Mesh(
        mesh.devices.reshape(mesh.shape["grp"], mesh.shape["row"] // 2, 2, mesh.shape["col"]),
        (X, Y, K, Z),
    )
    return jax.shard_map(
        per_device,
        mesh=torus,
        in_specs=(P(X, ROW, Z), P(X, ROW, Z), P(Z, None)),
        out_specs=(P(X, ROW, Z), P(Z, None), P(ROW, Z)),
        check_vma=False,
    )
```

```python
import functools
import math

import jax
import jax.numpy as jnp
from jax import lax
from jax.experimental import pallas as pl
from jax.experimental.pallas import tpu as pltpu
from jax.sharding import Mesh
from jax.sharding import PartitionSpec as P

MESH = pl.DeviceIdType.MESH
X, Y, K, Z = "grp", "row_0", "row_1", "col"
ROW = (Y, K)

momentum_decay = 0.9
ridge_scale = 0.0001
epsilon = 1e-06


def peer_of(axis, offset):
    return lax.rem(lax.axis_index(axis) + offset, lax.axis_size(axis))


def meet(axes, pairs=False):
    barrier = pltpu.get_barrier_semaphore()
    count = 0
    for axis in axes:
        for j in range(1, lax.axis_size(axis)):
            pl.semaphore_signal(barrier, inc=1, device_id={axis: peer_of(axis, j)}, device_id_type=MESH)
            count += 1
    for j in range(1, lax.axis_size(X) if pairs else 1):
        pl.semaphore_signal(barrier, inc=1, device_id={X: peer_of(X, j), K: peer_of(K, 1)}, device_id_type=MESH)
        count += 1
    return lambda: pl.semaphore_wait(barrier, count)


def send(src, dst, send_sem, recv_sem, axis, peer):
    copy = pltpu.make_async_remote_copy(
        src_ref=src, dst_ref=dst, send_sem=send_sem, recv_sem=recv_sem,
        device_id={axis: peer}, device_id_type=MESH,
    )
    copy.start()
    return copy


def scatter(tiles, arrived, sems, axis):
    copies = []
    for j in range(1, lax.axis_size(axis)):
        peer = peer_of(axis, j)
        copies.append(send(tiles.at[peer], arrived.at[j - 1], sems.at[0, j - 1], sems.at[1, j - 1], axis, peer))
    return copies


def share(slot, sems, axis):
    return [
        send(slot, slot, sems.at[0, j - 1], sems.at[1, j - 1], axis, peer_of(axis, j))
        for j in range(1, lax.axis_size(axis))
    ]


def share_pair(slot, sems):
    copies = []
    for j in range(lax.axis_size(X)):
        for i in range(2):
            if i + j:
                at = 2 * j + i - 1
                copy = pltpu.make_async_remote_copy(
                    src_ref=slot, dst_ref=slot, send_sem=sems.at[0, at], recv_sem=sems.at[1, at],
                    device_id={X: peer_of(X, j), K: peer_of(K, i)}, device_id_type=MESH,
                )
                copy.start()
                copies.append(copy)
    return copies


def arrive(copies):
    for copy in copies:
        copy.wait_recv()


def depart(copies):
    for copy in copies:
        copy.wait_send()


def left_kernel(
    mom, grad, basis, gram, left, low, part, xin, zpart, zin, lall, gall, gpair, kin, gy, gyin, gfull,
    sx, sz, sza, sxa, sk, sy, sgy, sgx, sgk,
):
    nx, ny, nz = lax.axis_size(X), lax.axis_size(Y), lax.axis_size(Z)
    g, y, k, c = (lax.axis_index(a) for a in (X, Y, K, Z))
    gathered = meet((X, Y, K, Z))
    chunks, lanes = part.shape[0], part.shape[3]
    tall = 4 * nz
    merged_low = (mom[...] + grad[...].astype(jnp.float32)).astype(jnp.bfloat16)
    low[...] = merged_low
    pending = []

    def started(copies):
        pending.extend(copies)
        return copies

    sent = []
    for t in range(chunks):
        product = jnp.dot(
            merged_low[t * tall : (t + 1) * tall], basis[...], preferred_element_type=jnp.float32
        )
        for b in range(nx):
            part[t, b] = product[:, b * lanes : (b + 1) * lanes]
        if t == 0:
            gathered()
        sent.append(started(scatter(part.at[t], xin.at[t], sx.at[t], X)))
    after = []
    for t in range(chunks):
        arrive(sent[t])
        total = part[t, g]
        for j in range(nx - 1):
            total = total + xin[t, j]
        for q in range(nz):
            zpart[t, q] = total[4 * q : 4 * q + 4]
        after.append(started(scatter(zpart.at[t], zin.at[t], sz.at[t], Z)))
    sent, after = after, []
    for t in range(chunks):
        arrive(sent[t])
        own = zpart[t, c]
        for j in range(nz - 1):
            own = own + zin[t, j]
        lall[t, g, c] = own
        after.append(started(share(lall.at[t, g, c], sza.at[t], Z)))
    sent, after = after, []
    for t in range(chunks):
        arrive(sent[t])
        after.append(started(share(lall.at[t, g], sxa.at[t], X)))
    for t in range(chunks):
        arrive(after[t])
        rows = slice(t * tall, (t + 1) * tall)
        for b in range(nx):
            for q in range(nz):
                left[t * tall + 4 * q : t * tall + 4 * q + 4, b * lanes : (b + 1) * lanes] = lall[t, b, q]
        mine = left[rows, pl.ds(pl.multiple_of(g * lanes, lanes), lanes)]
        outer = lax.dot_general(
            mine, left[rows, :], (((0,), (0,)), ((), ())),
            precision=lax.Precision.HIGHEST, preferred_element_type=jnp.float32,
        )
        gall[...] = outer if t == 0 else gall[...] + outer
    half = gall.shape[1] // 2
    parts, wide = gpair.shape[0], gpair.shape[3]
    deep = lanes // ny
    sent = []
    for u in range(parts):
        for h in range(2):
            lane = h * half + u * wide
            gpair[u, h] = gall[:, lane : lane + wide]
        sent.append(started(scatter(gpair.at[u], kin.at[u], sk.at[u], K)))
    after = []
    for u in range(parts):
        arrive(sent[u])
        total = gpair[u, k] + kin[u, 0]
        for p in range(ny):
            gy[u, p] = total[p * deep : (p + 1) * deep]
        after.append(started(scatter(gy.at[u], gyin.at[u], sy.at[u], Y)))
    sent, after = after, []
    for u in range(parts):
        arrive(sent[u])
        own = gy[u, y]
        for j in range(ny - 1):
            own = own + gyin[u, j]
        gfull[k, u, g, y] = own
        after.append(started(share(gfull.at[k, u, g, y], sgy.at[u], Y)))
    sent, after = after, []
    for u in range(parts):
        arrive(sent[u])
        after.append(started(share(gfull.at[k, u, g], sgx.at[u], X)))
    sent = []
    for u in range(parts):
        arrive(after[u])
        sent.append(started(share(gfull.at[k, u], sgk.at[u], K)))
    for u in range(parts):
        arrive(sent[u])
        for h in range(2):
            for b in range(nx):
                for p in range(ny):
                    at = b * lanes + p * deep
                    lane = h * half + u * wide
                    gram[at : at + deep, lane : lane + wide] = gfull[h, u, b, p]
    depart(pending)


def copies_of(count, n):
    return pltpu.SemaphoreType.DMA((count, 2, n - 1) if count else (2, n - 1))


def left_call(mom, grad, basis):
    nx, ny, nz = lax.axis_size(X), lax.axis_size(Y), lax.axis_size(Z)
    rows, cols = mom.shape
    rank = basis.shape[1]
    lanes = rank // nx
    chunks = rows // (4 * nz)
    half = rank // 2
    f32 = jnp.float32
    vmem = pl.BlockSpec(memory_space=pltpu.VMEM)
    return pl.pallas_call(
        left_kernel,
        out_shape=(
            jax.ShapeDtypeStruct((rank, rank), f32),
            jax.ShapeDtypeStruct((rows, rank), f32),
            jax.ShapeDtypeStruct((rows, cols), jnp.bfloat16),
        ),
        in_specs=[vmem] * 3,
        out_specs=(vmem,) * 3,
        scratch_shapes=[
            pltpu.VMEM((chunks, nx, 4 * nz, lanes), f32),
            pltpu.VMEM((chunks, nx - 1, 4 * nz, lanes), f32),
            pltpu.VMEM((chunks, nz, 4, lanes), f32),
            pltpu.VMEM((chunks, nz - 1, 4, lanes), f32),
            pltpu.VMEM((chunks, nx, nz, 4, lanes), f32),
            pltpu.VMEM((lanes, rank), f32),
            pltpu.VMEM((2, 2, lanes, half // 2), f32),
            pltpu.VMEM((2, 1, lanes, half // 2), f32),
            pltpu.VMEM((2, ny, lanes // ny, half // 2), f32),
            pltpu.VMEM((2, ny - 1, lanes // ny, half // 2), f32),
            pltpu.VMEM((2, 2, nx, ny, lanes // ny, half // 2), f32),
            copies_of(chunks, nx), copies_of(chunks, nz), copies_of(chunks, nz), copies_of(chunks, nx),
            copies_of(2, 2), copies_of(2, ny), copies_of(2, ny), copies_of(2, nx), copies_of(2, 2),
        ],
        compiler_params=pltpu.CompilerParams(collective_id=0, has_side_effects=True, vmem_limit_bytes=24 << 20),
        name="left",
    )(mom, grad, basis)


def right_kernel(
    groups, whole_rows, low, orth, nb_out, rms_out, ksend, kin, mine, xsend, xin, ysum, ysend, yin, nb, low_left,
    qz, qx, qy, sk, sx, sy, say, sax, sak, sqz, sqx, sqy,
):
    nx, ny, nz = lax.axis_size(X), lax.axis_size(Y), lax.axis_size(Z)
    g, y, k, c = (lax.axis_index(a) for a in (X, Y, K, Z))
    gathered = meet((X, Y, K, Z), True)
    chunks, half, wide = ksend.shape
    f32, bf16 = jnp.float32, jnp.bfloat16
    low_left[...] = orth[...].astype(bf16)
    pending = []

    def started(copies):
        pending.extend(copies)
        return copies

    def product(at):
        return lax.dot_general(
            low[:, pl.ds(pl.multiple_of(at, 128), 128)], low_left[...], (((0,), (0,)), ((), ())),
            preferred_element_type=f32,
        ) * (1.0 / groups)

    @pl.loop(0, half // 128)
    def _(i):
        tile = product((1 - k) * half + i * 128).astype(bf16)
        for t in range(chunks):
            ksend[t, pl.ds(pl.multiple_of(i * 128, 128), 128), :] = tile[:, t * wide : (t + 1) * wide]

    @pl.loop(0, half // 128)
    def _(i):
        tile = product(k * half + i * 128)
        for t in range(chunks):
            mine[t, pl.ds(pl.multiple_of(i * 128, 128), 128), :] = tile[:, t * wide : (t + 1) * wide]

    gathered()
    sent = [
        started([send(ksend.at[t], kin.at[t], sk.at[t, 0, 0], sk.at[t, 1, 0], K, 1 - k)]) for t in range(chunks)
    ]

    block = half // nx
    piece_rows = block // ny
    after = []
    for t in range(chunks):
        arrive(sent[t])
        for b in range(nx):
            at = slice(b * block, (b + 1) * block)
            both = mine[t, at] + kin[t, at].astype(f32)
            mine[t, at] = both
            xsend[t, b] = both.astype(bf16)
        after.append(started(scatter(xsend.at[t], xin.at[t], sx.at[t], X)))
    sent, after = after, []
    for t in range(chunks):
        arrive(sent[t])
        total = mine[t, pl.ds(pl.multiple_of(g * block, block), block), :]
        for j in range(nx - 1):
            total = total + xin[t, j].astype(f32)
        ysum[t] = total
        for b in range(ny):
            ysend[t, b] = total[b * piece_rows : (b + 1) * piece_rows].astype(bf16)
        after.append(started(scatter(ysend.at[t], yin.at[t], sy.at[t], Y)))
    sent, after = after, []
    for t in range(chunks):
        arrive(sent[t])
        piece = ysum[t, pl.ds(pl.multiple_of(y * piece_rows, 8), piece_rows), :]
        for j in range(ny - 1):
            piece = piece + yin[t, j].astype(f32)
        nb[t, k, g, y] = piece.astype(bf16)
        qz[c, :, t * wide : (t + 1) * wide] = jnp.sum(piece * piece, axis=0, keepdims=True)
        if t == chunks - 1:
            sent_q = started(share(qz.at[c], sqz, Z))
        after.append(started(share(nb.at[t, k, g, y], say.at[t], Y)))

    def summed(ref, n):
        acc = ref[0]
        for j in range(1, n):
            acc = acc + ref[j]
        return acc

    sent, after = after, []
    for t in range(chunks):
        arrive(sent[t])
        after.append(started(share(nb.at[t, k, g], sax.at[t], X)))
    arrive(sent_q)
    qy[y] = summed(qz, nz)
    sent_q = started(share(qy.at[y], sqy, Y))
    sent = []
    for t in range(chunks - 1):
        arrive(after[t])
        sent.append(started(share(nb.at[t, k], sak.at[t], K)))
    arrive(sent_q)
    qx[2 * g + k] = summed(qy, ny)
    sent_q = started(share_pair(qx.at[2 * g + k], sqx))
    arrive(after[-1])
    sent.append(started(share(nb.at[chunks - 1, k], sak.at[chunks - 1], K)))
    for t in range(chunks):
        arrive(sent[t])
        for h in range(2):
            for b in range(nx):
                for p in range(ny):
                    at = h * half + b * block + p * piece_rows
                    nb_out[t, at : at + piece_rows, :] = nb[t, h, b, p]
    arrive(sent_q)
    rms_out[...] = jnp.sqrt(summed(qx, 2 * nx) / whole_rows + epsilon)
    depart(pending)


def right_call(low, orth):
    nx, ny, nz = lax.axis_size(X), lax.axis_size(Y), lax.axis_size(Z)
    rows, cols = low.shape
    rank = orth.shape[1]
    half = cols // 2
    block = half // nx
    piece = block // ny
    wide = 128
    chunks = rank // wide
    f32, bf16 = jnp.float32, jnp.bfloat16
    vmem = pl.BlockSpec(memory_space=pltpu.VMEM)
    return pl.pallas_call(
        functools.partial(right_kernel, nx, cols * nz),
        out_shape=(
            jax.ShapeDtypeStruct((chunks, cols, wide), bf16),
            jax.ShapeDtypeStruct((1, rank), f32),
        ),
        in_specs=[vmem] * 2,
        out_specs=(vmem,) * 2,
        scratch_shapes=[
            pltpu.VMEM((chunks, half, wide), bf16),
            pltpu.VMEM((chunks, half, wide), bf16),
            pltpu.VMEM((chunks, half, wide), f32),
            pltpu.VMEM((chunks, nx, block, wide), bf16),
            pltpu.VMEM((chunks, nx - 1, block, wide), bf16),
            pltpu.VMEM((chunks, block, wide), f32),
            pltpu.VMEM((chunks, ny, piece, wide), bf16),
            pltpu.VMEM((chunks, ny - 1, piece, wide), bf16),
            pltpu.VMEM((chunks, 2, nx, ny, piece, wide), bf16),
            pltpu.VMEM((rows, rank), bf16),
            pltpu.VMEM((nz, 1, rank), f32),
            pltpu.VMEM((2 * nx, 1, rank), f32),
            pltpu.VMEM((ny, 1, rank), f32),
            copies_of(chunks, 2), copies_of(chunks, nx), copies_of(chunks, ny), copies_of(chunks, ny),
            copies_of(chunks, nx), copies_of(chunks, 2),
            copies_of(0, nz), copies_of(0, 2 * nx), copies_of(0, ny),
        ],
        compiler_params=pltpu.CompilerParams(collective_id=1, has_side_effects=True, vmem_limit_bytes=24 << 20),
        name="right",
    )(low, orth)


def final_kernel(update_scale, nb, rms, orth, mom, grad, newmom, basis, update, stack):
    rows = mom.shape[0]
    chunks, wide = nb.shape[0], nb.shape[2]
    f32, bf16 = jnp.float32, jnp.bfloat16

    @pl.when(pl.program_id(0) == 0)
    def _():
        stack[:rows] = orth[...].astype(bf16)
        stack[rows:] = (orth[...] * rms[...]).astype(bf16)

    inverse = 1.0 / rms[...]
    for t in range(chunks):
        at = slice(t * wide, (t + 1) * wide)
        basis[:, at] = (nb[t].astype(f32) * inverse[:, at]).astype(bf16)
    both = lax.dot_general(stack[...], basis[...], (((1,), (1,)), ((), ())), preferred_element_type=f32)
    update[...] = (update_scale * both[:rows]).astype(bf16)
    newmom[...] = mom[...] + grad[...].astype(f32) - (1 - momentum_decay) * both[rows:]


def final_call(nb, rms, orth, mom, grad, update_scale):
    chunks, cols, wide = nb.shape
    rows, rank = orth.shape
    step = 512
    f32, bf16 = jnp.float32, jnp.bfloat16
    strip = pl.BlockSpec((rows, step), lambda i: (0, i))
    return pl.pallas_call(
        functools.partial(final_kernel, update_scale),
        grid=(cols // step,),
        out_shape=(
            jax.ShapeDtypeStruct((rows, cols), f32),
            jax.ShapeDtypeStruct((cols, rank), bf16),
            jax.ShapeDtypeStruct((rows, cols), bf16),
        ),
        in_specs=[
            pl.BlockSpec((chunks, step, wide), lambda i: (0, i, 0)),
            pl.BlockSpec((1, rank), lambda i: (0, 0)),
            pl.BlockSpec((rows, rank), lambda i: (0, 0)),
            strip,
            strip,
        ],
        out_specs=(strip, pl.BlockSpec((step, rank), lambda i: (i, 0)), strip),
        scratch_shapes=[pltpu.VMEM((2 * rows, rank), bf16)],
        compiler_params=pltpu.CompilerParams(vmem_limit_bytes=16 << 20),
        name="final",
    )(nb, rms, orth, mom, grad)


def factor_kernel(gram, left, orth, a, diag):
    f32 = jnp.float32
    rank = gram.shape[0]
    rows = left.shape[0]
    size = 128
    sub = lax.broadcasted_iota(jnp.int32, (8, size), 0)
    lane = lax.broadcasted_iota(jnp.int32, (8, size), 1)
    at_row = lax.broadcasted_iota(jnp.int32, (size, size), 0)
    at_col = lax.broadcasted_iota(jnp.int32, (size, size), 1)
    trace = jnp.zeros((size, size), f32)
    for b in range(rank // size):
        s = slice(b * size, (b + 1) * size)
        trace = trace + jnp.where(at_row == at_col, gram[s, s], 0.0)
    shift = ridge_scale * (jnp.sum(trace) / rank)
    a[:rank] = gram[...]
    for b in range(rank // size):
        s = slice(b * size, (b + 1) * size)
        a[s, s] = gram[s, s] + jnp.where(at_row == at_col, shift, 0.0)
    a[rank:] = left[...]

    def spread(v, l):
        return jnp.broadcast_to(v[:, l : l + 1], (8, size))

    def everywhere(v, i):
        return jnp.broadcast_to(v[i : i + 1, :], (8, size))

    def folded(v):
        return jnp.broadcast_to(jnp.sum(v, axis=0, keepdims=True), (8, size))

    def packed(lines):
        out = lines[0]
        for i in range(1, 8):
            out = jnp.where(sub == i, lines[i], out)
        return out

    def dot(x, y):
        return lax.dot_general(
            x, y, (((1,), (1,)), ((), ())), precision=lax.Precision.HIGHEST, preferred_element_type=f32
        )

    @pl.loop(0, rank // size)
    def _(block):
        off = pl.multiple_of(block * size, size)
        diag[0] = a[pl.ds(off, size), pl.ds(off, size)]
        upper, inverse = [], []
        for s in range(size // 8):
            base = 8 * s
            lines, other = [], []
            for i in range(8):
                line = jnp.broadcast_to(diag[0, base + i : base + i + 1, :], (8, size))
                unit = jnp.where(lane == base + i, 1.0, 0.0)
                if s:
                    acc_u = acc_w = None
                    for t in range(s):
                        factor = spread(upper[t], base + i)
                        u, w = factor * upper[t], factor * inverse[t]
                        acc_u = u if acc_u is None else acc_u + u
                        acc_w = w if acc_w is None else acc_w + w
                    line = line - folded(acc_u)
                    unit = unit - folded(acc_w)
                lines.append(line)
                other.append(unit)
            panel = packed(lines)
            cols = [spread(panel, base + j) for j in range(8)]
            d = [[everywhere(cols[j], i) if j >= i else None for j in range(8)] for i in range(8)]
            for j in range(8):
                scale = lax.rsqrt(d[j][j])
                lines[j] = lines[j] * scale
                other[j] = other[j] * scale
                u = [None] * 8
                for i in range(j + 1, 8):
                    u[i] = d[j][i] * scale
                for i in range(j + 1, 8):
                    for m in range(i, 8):
                        d[i][m] = d[i][m] - u[i] * u[m]
                for i in range(j + 1, 8):
                    lines[i] = lines[i] - u[i] * lines[j]
                    other[i] = other[i] - u[i] * other[j]
            upper.append(packed(lines))
            inverse.append(packed(other))
            diag[1, base : base + 8, :] = inverse[s]
        for b in range(rank // size):

            @pl.when(block == b)
            def _():
                at, after = b * size, (b + 1) * size
                below = dot(a[after:, at:after], diag[1])
                a[after:, at:after] = below
                if after < rank:
                    a[after:, after:] = a[after:, after:] - dot(below, below[: rank - after])

    orth[...] = a[rank:]


def factor_call(gram, left):
    rank, rows = gram.shape[0], left.shape[0]
    vmem = pl.BlockSpec(memory_space=pltpu.VMEM)
    return pl.pallas_call(
        factor_kernel,
        out_shape=jax.ShapeDtypeStruct((rows, rank), jnp.float32),
        in_specs=[vmem] * 2,
        out_specs=vmem,
        scratch_shapes=[pltpu.VMEM((rank + rows, rank), jnp.float32), pltpu.VMEM((2, 128, 128), jnp.float32)],
        compiler_params=pltpu.CompilerParams(vmem_limit_bytes=16 << 20),
        name="factor",
    )(gram, left)


def per_device(gradients, momentum, right_basis):
    mom, grad = momentum[0], gradients[0]
    rank = right_basis.shape[1]
    whole_rows = mom.shape[0] * lax.axis_size(Y) * lax.axis_size(K)
    gram_matrix, left_factor, merged_low = left_call(mom, grad, right_basis)
    orthonormal = factor_call(gram_matrix, left_factor)
    gathered, column_rms = right_call(merged_low, orthonormal)
    new_momentum, new_basis, update = final_call(
        gathered, column_rms, orthonormal, mom, grad, math.sqrt(whole_rows / rank)
    )
    return new_momentum[None], new_basis, update


def solution(mesh):
    torus = Mesh(
        mesh.devices.reshape(mesh.shape["grp"], mesh.shape["row"] // 2, 2, mesh.shape["col"]),
        (X, Y, K, Z),
    )
    return jax.shard_map(
        per_device,
        mesh=torus,
        in_specs=(P(X, ROW, Z), P(X, ROW, Z), P(Z, None)),
        out_specs=(P(X, ROW, Z), P(Z, None), P(ROW, Z)),
        check_vma=False,
    )
```
